32 devices in a mesh: dp: 4 (over x, y), tp: 8 (over z, core).
Axes of the slice: x: 2, y: 2, z: 4, core: 2. Of those that a mesh axis runs over, the one named last changes fastest.
Arguments:
- x: bfloat16 [4096, 12288], P(('dp', 'tp')), parts along dimension 0
- gain: bfloat16 [12288], replicated
- wq: bfloat16 [12288, 12288], P(None, 'tp')
- wk: bfloat16 [12288, 12288], P(None, 'tp')
- wv: bfloat16 [12288, 12288], P(None, 'tp')
- wo: bfloat16 [12288, 12288], P('tp')
Outputs:
- output: bfloat16 [4096, 12288], P(('dp', 'tp')), parts along dimension 0
There are 4 independent parts. The reference program is written for one: setup_inputs(seed, part) draws one part's arguments, and reference() takes and returns one part's arrays. A program takes and returns all parts, laid end to end along the dimension named above; an argument that names none is the same for every part.
All inputs are finite; a program needn't handle non-finite values.
Results may differ from the reference program's by a relative error of at most 0.012.
Values are sent between devices in bfloat16 or wider.
A program may use at most 2 GiB of HBM per device.

```python
import jax
import jax.numpy as jnp
from jax import lax

ROWS = 1024
D = 12288
HEADS = 96
KV_HEADS = 96
HEAD = 128
THETA = 10000


def setup_inputs(seed: int = 0, part: int = 0) -> dict:
    kx, kn, kq, kk, kv, ko = jax.random.split(jax.random.key(seed), 6)

    def weights(key, rows, columns):
        return jax.random.normal(key, (rows, columns), jnp.float32) * rows**-0.5

    drawn = {
        "x": jax.random.normal(jax.random.fold_in(kx, part), (ROWS, D), jnp.float32),
        "gain": 1 + 0.1 * jax.random.normal(kn, (D,), jnp.float32),
        "wq": 2 * weights(kq, D, HEADS * HEAD),
        "wk": 2 * weights(kk, D, KV_HEADS * HEAD),
        "wv": 4 * weights(kv, D, KV_HEADS * HEAD),
        "wo": weights(ko, HEADS * HEAD, D),
    }
    return {k: v.astype(jnp.bfloat16) for k, v in drawn.items()}


def normed(x, gain):
    wide = x.astype(jnp.float32)
    scale = lax.rsqrt(jnp.mean(wide * wide, -1, keepdims=True) + 1e-6)
    return (wide * scale * gain.astype(jnp.float32)).astype(jnp.bfloat16)


def turned(t, place, theta):
    half = t.shape[-1] // 2
    angle = place.astype(jnp.float32)[:, None] * theta ** (-jnp.arange(half, dtype=jnp.float32) / half)
    cos, sin = jnp.cos(angle)[:, None], jnp.sin(angle)[:, None]
    a, b = t[..., :half].astype(jnp.float32), t[..., half:].astype(jnp.float32)
    return jnp.concatenate([a * cos - b * sin, b * cos + a * sin], -1).astype(jnp.bfloat16)


def matmul(a, w):
    return jnp.dot(a, w, preferred_element_type=jnp.float32).astype(jnp.bfloat16)


def einsum(form, a, b):
    return jnp.einsum(form, a.astype(jnp.float32), b.astype(jnp.float32))


def attention(q, k, v):
    scores = einsum("tgsd,ugd->gstu", q, k) * q.shape[-1] ** -0.5
    token = jnp.arange(q.shape[0])
    scores = jnp.where(token[:, None] >= token, scores, -jnp.inf)
    weights = jax.nn.softmax(scores, -1).astype(jnp.bfloat16)
    return einsum("gstu,ugd->tgsd", weights, v).astype(jnp.bfloat16)


def reference(x, gain, wq, wk, wv, wo):
    a, place = normed(x, gain), jnp.arange(ROWS)
    q = turned(matmul(a, wq).reshape(ROWS, HEADS, HEAD), place, THETA).reshape(ROWS, KV_HEADS, -1, HEAD)
    k = turned(matmul(a, wk).reshape(ROWS, KV_HEADS, HEAD), place, THETA)
    v = matmul(a, wv).reshape(ROWS, KV_HEADS, HEAD)
    seen = attention(q, k, v).reshape(ROWS, HEADS * HEAD)
    return (x.astype(jnp.float32) + jnp.dot(seen, wo, preferred_element_type=jnp.float32)).astype(jnp.bfloat16)
```

```python
import functools

import jax
import jax.numpy as jnp
from jax import lax
from jax.experimental import pallas as pl
from jax.experimental.pallas import tpu as pltpu
from jax.sharding import PartitionSpec as P

HEAD = 128
THETA = 10000
D = 12288
ROWS = 1024
OWN = 128
PAIR = 256
CHIPS = 4
WIDE = 1536
HEADS = 12
CHUNK = 16
NCH = OWN // CHUNK
TN = 512
TK = 3072
NK = D // TK
NT = 3 * WIDE // TN
PER = WIDE // TN
TO = 1024
NO = D // TO
GROUP = 4
BLOCK = 256
LOG2E = 1.4426950408889634
HIDDEN = -2e30
MESH = pl.DeviceIdType.MESH
F32, BF16 = jnp.float32, jnp.bfloat16


def _dot(a, b, ca, cb):
    return lax.dot_general(a, b, (((ca,), (cb,)), ((), ())), preferred_element_type=F32)


def _loop(n, body):
    lax.fori_loop(0, n, lambda i, _: body(i), None)


def _kernel(x_ref, gain_ref, cos_ref, sin_ref, wq_ref, wk_ref, wv_ref, wo_ref, y_ref, all_ref, wring, xbuf, kbuf, vbuf, qbuf, seen, oring, up, acc,
            stage, sib, mix_s, top_s, wsem, osem, lsem, arrive, pair_recv, pair_send, line_send, sum_recv, sum_send, sib_recv, sib_send, ysem, xsem, free):
    tp = lax.axis_index("tp")
    z, c = lax.div(tp, 2), lax.rem(tp, 2)
    me_sib = {"tp": 2 * z + 1 - c}
    right = {"tp": jnp.minimum(tp + 2, 7)}
    left = {"tp": jnp.maximum(tp - 2, 0)}
    inner = (z > 0) & (z < 3)

    def fetch(nt, kc):
        which, col = lax.div(nt, PER), pl.multiple_of(lax.rem(nt, PER) * TN, TN)
        for p, w in enumerate((wq_ref, wk_ref, wv_ref)):
            @pl.when(which == p)
            def _():
                pltpu.make_async_copy(w.at[pl.ds(kc * TK, TK), pl.ds(col, TN)], wring.at[kc], wsem.at[kc]).start()

    def fetch_o(j, slot):
        return pltpu.make_async_copy(wo_ref.at[:, pl.ds(pl.multiple_of(j * TO, TO), TO)], oring.at[slot], osem.at[slot])

    own_x = pltpu.make_async_copy(x_ref, xbuf.at[pl.ds(0, OWN)], xsem)
    own_x.start()
    for kc in range(NK):
        fetch(0, kc)
    for j in range(2):
        fetch_o(j, j).start()

    def rows(s, i):
        return all_ref.at[pl.ds(pl.multiple_of(s * PAIR + c * OWN + i * CHUNK, CHUNK), CHUNK)]

    def to_sib(s, i):
        return pltpu.make_async_remote_copy(src_ref=rows(s, i), dst_ref=rows(s, i), send_sem=pair_send.at[s], recv_sem=pair_recv.at[s],
                                            device_id=me_sib, device_id_type=MESH)

    def along(s, i, way):
        return pltpu.make_async_remote_copy(src_ref=rows(s, i), dst_ref=rows(s, i), send_sem=line_send.at[way, s], recv_sem=arrive.at[s, i],
                                            device_id=left if way else right, device_id_type=MESH)

    def handle(s, i):
        along(s, i, 0).wait_recv()

        @pl.when((s < z) & (z < 3))
        def _():
            along(s, i, 0).start()

        @pl.when((s > z) & (z > 0))
        def _():
            along(s, i, 1).start()

        to_sib(s, i).start()

    barrier = pltpu.get_barrier_semaphore()
    pl.semaphore_signal(barrier, inc=1, device_id=me_sib, device_id_type=MESH)

    @pl.when(z < 3)
    def _():
        pl.semaphore_signal(barrier, inc=1, device_id=right, device_id_type=MESH)

    @pl.when(z > 0)
    def _():
        pl.semaphore_signal(barrier, inc=1, device_id=left, device_id_type=MESH)

    @pl.when(inner)
    def _():
        pl.semaphore_wait(barrier, 3)

    @pl.when(jnp.logical_not(inner))
    def _():
        pl.semaphore_wait(barrier, 2)

    own_x.wait()

    def keep(i):
        return pltpu.make_async_copy(xbuf.at[pl.ds(pl.multiple_of(OWN + i * CHUNK, CHUNK), CHUNK)], rows(z, i), lsem)

    def send_own(i):
        to_sib(z, i).start()

        @pl.when(z > 0)
        def _():
            along(z, i, 1).start()

        @pl.when(z == 0)
        def _():
            along(z, i, 0).start()

    def norm(i):
        wide = xbuf[pl.ds(pl.multiple_of(i * CHUNK, CHUNK), CHUNK), :].astype(F32)
        scale = lax.rsqrt(jnp.mean(wide * wide, -1, keepdims=True) + 1e-6)
        out = (wide * scale * gain_ref[...].astype(F32)).astype(BF16)

        @pl.when(i > 0)
        def _():
            keep(i - 1).wait()
            send_own(i - 1)

        xbuf[pl.ds(pl.multiple_of(OWN + i * CHUNK, CHUNK), CHUNK), :] = out
        keep(i).start()

    _loop(NCH, norm)
    keep(NCH - 1).wait()
    send_own(NCH - 1)

    def first(i):
        @pl.when(z > 0)
        def _():
            handle(0, i)

        @pl.when(z == 1)
        def _():
            handle(2, i)

        @pl.when(z == 2)
        def _():
            handle(3, i)

    _loop(NCH, first)

    @pl.when(z == 1)
    def _():
        _loop(NCH, lambda i: along(1, i, 0).start())

    def project(s):
        @pl.when(((z == 0) & (s > 0)) | ((z == 3) & ((s == 1) | (s == 2))))
        def _():
            _loop(NCH, lambda i: handle(s, i))

        @pl.when((z == 2) & (s == 1))
        def _():
            _loop(NCH // 2, lambda i: handle(1, NCH // 2 + i))
            _loop(NCH, lambda i: along(2, i, 0).start())

        block = all_ref.at[pl.ds(pl.multiple_of(s * PAIR + (1 - c) * OWN, OWN), OWN)]
        pltpu.make_async_remote_copy(src_ref=block, dst_ref=block, send_sem=pair_send.at[s], recv_sem=pair_recv.at[s],
                                     device_id=me_sib, device_id_type=MESH).wait_recv()
        here = pl.ds(pl.multiple_of(s * PAIR, PAIR), PAIR)
        load = pltpu.make_async_copy(all_ref.at[here], xbuf, xsem)
        load.start()
        load.wait()

        def tile(nt):
            total = None
            for kc in range(NK):
                pltpu.make_async_copy(wq_ref.at[pl.ds(0, TK), pl.ds(0, TN)], wring.at[kc], wsem.at[kc]).wait()
                part = _dot(xbuf[:, kc * TK : (kc + 1) * TK], wring[kc], 1, 0)
                total = part if total is None else total + part

                @pl.when((s < CHIPS - 1) | (nt < NT - 1))
                def _():
                    fetch(lax.rem(nt + 1, NT), kc)

            t = total.astype(BF16)
            which, col = lax.div(nt, PER), lax.rem(nt, PER) * TN

            @pl.when(which < 2)
            def _():
                cos, sin = cos_ref[here, :], sin_ref[here, :]
                for n in range(TN // HEAD):
                    one = t[:, n * HEAD : (n + 1) * HEAD].astype(F32)
                    one = (one * cos + pltpu.roll(one, HEAD // 2, 1) * sin).astype(BF16)
                    at = pl.ds(pl.multiple_of(col + n * HEAD, HEAD), HEAD)

                    @pl.when(which == 0)
                    def _():
                        qbuf[:, at] = one

                    @pl.when(which == 1)
                    def _():
                        kbuf[here, at] = one

            @pl.when(which == 2)
            def _():
                for n in range(TN // HEAD):
                    at = pl.ds(pl.multiple_of(col + n * HEAD, HEAD), HEAD)
                    vbuf[at, here] = t[:, n * HEAD : (n + 1) * HEAD].T

            odd = lax.rem(nt, 2) == 1

            @pl.when((z == 1) & (s == 0) & odd & (nt >= 3))
            def _():
                handle(3, lax.div(nt - 3, 2))

            @pl.when((z == 2) & (s == 0) & odd & (nt >= 3))
            def _():
                handle(1, lax.div(nt - 3, 2))

            @pl.when((z == 1) & (s == 1) & odd)
            def _():
                handle(3, lax.div(nt - 1, 2) + NCH // 2)

        _loop(NT, tile)

    def attend(s):
        e = HEAD**-0.5 * LOG2E
        ones = jnp.ones((8, BLOCK), BF16)

        def group(g):
            ats = [pl.ds(pl.multiple_of((g * GROUP + n) * HEAD, HEAD), HEAD) for n in range(GROUP)]

            def block(j, diagonal):
                keys = pl.ds(pl.multiple_of(j * BLOCK, BLOCK), BLOCK)
                scores = [_dot(kbuf[keys, at], qbuf[:, at], 1, 1) for at in ats]
                weights, keeps = [], []
                if diagonal:
                    ok = lax.broadcasted_iota(jnp.int32, (BLOCK, PAIR), 1) >= lax.broadcasted_iota(jnp.int32, (BLOCK, PAIR), 0)
                for n, sc in enumerate(scores):
                    if diagonal:
                        sc = jnp.where(ok, sc, HIDDEN)
                        top = sc.max(axis=0, keepdims=True)
                    else:
                        old = top_s[n : n + 1, :]
                        top = jnp.maximum(old, sc.max(axis=0, keepdims=True))
                        keeps.append(jnp.exp2((old - top) * e))
                    top_s[n : n + 1, :] = top
                    weights.append(jnp.exp2((sc - top) * e).astype(BF16))
                for n, (at, p) in enumerate(zip(ats, weights)):
                    values = jnp.concatenate([vbuf[at, keys], ones], axis=0)
                    new = _dot(values, p, 1, 0)
                    mix_s[n] = new if diagonal else mix_s[n] * keeps[n] + new

            block(s, True)
            lax.fori_loop(0, s, lambda j, _: block(j, False), None)
            for n, at in enumerate(ats):
                out = mix_s[n, :HEAD, :] * (1 / mix_s[n, HEAD : HEAD + 1, :])
                seen[pl.ds(pl.multiple_of(s * PAIR, PAIR), PAIR), at] = out.T.astype(BF16)

        _loop(HEADS // GROUP, group)

        @pl.when((z == 1) & (s == 0))
        def _():
            handle(3, NCH // 2 - 1)

        @pl.when((z == 2) & (s == 0))
        def _():
            handle(1, NCH // 2 - 1)

    def output(s, n):
        last = s == z
        ours = pl.ds(pl.multiple_of(c * OWN, OWN), OWN)
        theirs = pl.ds(pl.multiple_of((1 - c) * OWN, OWN), OWN)
        from_near = jnp.where(last, z < 3, inner)
        from_left = last & (z > 0)
        target = jnp.where((z + 1 == s), CHIPS, s)

        def swap(j):
            return pltpu.make_async_remote_copy(src_ref=stage.at[lax.rem(j, 4)], dst_ref=sib.at[j], send_sem=sib_send.at[lax.rem(j, 4)],
                                                recv_sem=sib_recv.at[j], device_id=me_sib, device_id_type=MESH)

        def onward(j, to):
            return pltpu.make_async_remote_copy(src_ref=up.at[s, j], dst_ref=up.at[target, j], send_sem=sum_send.at[s], recv_sem=sum_recv.at[target, j],
                                                device_id=to, device_id_type=MESH)

        def arrived(slot, j):
            pltpu.make_async_remote_copy(src_ref=up.at[slot, j], dst_ref=up.at[slot, j], send_sem=sum_send.at[s], recv_sem=sum_recv.at[slot, j],
                                         device_id=right, device_id_type=MESH).wait_recv()

        @pl.when(n > 0)
        def _():
            pl.semaphore_wait(free, 1)

        def step(j):
            @pl.when(j < NO)
            def _():
                slot = lax.rem(j, 2)
                fetch_o(0, slot).wait()

                @pl.when(j >= 4)
                def _():
                    swap(j).wait_send()

                a = lax.rem(j, 3)
                acc[a] = _dot(seen[pl.ds(pl.multiple_of(s * PAIR, PAIR), PAIR), :], oring[slot], 1, 0)
                stage[lax.rem(j, 4)] = acc[a, theirs, :].astype(BF16)

                @pl.when((n < 3) | (j < NO - 2))
                def _():
                    fetch_o(lax.rem(j + 2, NO), slot).start()

            @pl.when((j >= 2) & (j < NO + 2))
            def _():
                f = j - 2
                a = lax.rem(f, 3)
                pltpu.make_async_remote_copy(src_ref=stage.at[0], dst_ref=sib.at[f], send_sem=sib_send.at[0], recv_sem=sib_recv.at[f],
                                             device_id=me_sib, device_id_type=MESH).wait_recv()
                acc[a, ours, :] = acc[a, ours, :] + sib[f].astype(F32)

                @pl.when(from_near)
                def _():
                    arrived(s, f)
                    acc[a, ours, :] = acc[a, ours, :] + up[s, f].astype(F32)

                @pl.when(from_left)
                def _():
                    arrived(CHIPS, f)
                    acc[a, ours, :] = acc[a, ours, :] + up[CHIPS, f].astype(F32)

                up[s, f] = acc[a, ours, :].astype(BF16)

            @pl.when(j < NO)
            def _():
                swap(j).start()

            @pl.when(j >= 3)
            def _():
                f = j - 3

                @pl.when(z > s)
                def _():
                    onward(f, left).start()

                @pl.when(z < s)
                def _():
                    onward(f, right).start()

                @pl.when(last)
                def _():
                    pltpu.make_async_copy(up.at[s, f], y_ref.at[:, pl.ds(pl.multiple_of(f * TO, TO), TO)], ysem).start()

        _loop(NO + 3, step)
        for j in range(NO - 4, NO):
            swap(j).wait_send()

        @pl.when(n < 3)
        def _():
            pl.semaphore_signal(free, inc=1, device_id=me_sib, device_id_type=MESH)

    start = jnp.where(z == 0, 1, jnp.where(z == 1, 3, jnp.where(z == 2, 2, 0)))

    def turn(st):
        @pl.when(st < CHIPS)
        def _():
            project(st)
            attend(st)

        n = st - start

        @pl.when((n >= 0) & (n < 4))
        def _():
            order1 = jnp.where(n == 0, 2, jnp.where(n == 1, 0, jnp.where(n == 2, 3, 1)))
            order2 = jnp.where(n < 2, n, 5 - n)
            s = jnp.where(z == 0, lax.rem(n + 1, 4), jnp.where(z == 1, order1, jnp.where(z == 2, order2, n)))
            output(s, n)

    _loop(7, turn)

    def drain(s):
        block = all_ref.at[pl.ds(0, OWN)]
        pltpu.make_async_remote_copy(src_ref=block, dst_ref=block, send_sem=pair_send.at[s], recv_sem=pair_recv.at[s],
                                     device_id=me_sib, device_id_type=MESH).wait_send()

        @pl.when((s <= z) & (z < 3))
        def _():
            pltpu.make_async_remote_copy(src_ref=block, dst_ref=block, send_sem=line_send.at[0, s], recv_sem=pair_recv.at[s],
                                         device_id=right, device_id_type=MESH).wait_send()

        @pl.when((s >= z) & (z > 0))
        def _():
            pltpu.make_async_remote_copy(src_ref=block, dst_ref=block, send_sem=line_send.at[1, s], recv_sem=pair_recv.at[s],
                                         device_id=left, device_id_type=MESH).wait_send()

        @pl.when(s != z)
        def _():
            pltpu.make_async_remote_copy(src_ref=up.at[s], dst_ref=up.at[s], send_sem=sum_send.at[s], recv_sem=sum_recv.at[s, 0],
                                         device_id=right, device_id_type=MESH).wait_send()

    _loop(CHIPS, drain)
    pltpu.make_async_copy(all_ref.at[pl.ds(0, OWN)], y_ref, ysem).wait()


def layer(x, gain, cos, sin, wq, wk, wv, wo):
    anywhere, vmem = pl.BlockSpec(memory_space=pl.ANY), pl.BlockSpec(memory_space=pltpu.VMEM)
    dma = pltpu.SemaphoreType.DMA
    y, _ = pl.pallas_call(
        _kernel,
        in_specs=[anywhere, vmem, vmem, vmem, anywhere, anywhere, anywhere, anywhere],
        out_specs=[anywhere, anywhere],
        out_shape=[jax.ShapeDtypeStruct((OWN, D), BF16), jax.ShapeDtypeStruct((ROWS, D), BF16)],
        scratch_shapes=[
            pltpu.VMEM((NK, TK, TN), BF16),
            pltpu.VMEM((PAIR, D), BF16),
            pltpu.VMEM((ROWS, WIDE), BF16),
            pltpu.VMEM((WIDE, ROWS), BF16),
            pltpu.VMEM((PAIR, WIDE), BF16),
            pltpu.VMEM((ROWS, WIDE), BF16),
            pltpu.VMEM((2, WIDE, TO), BF16),
            pltpu.VMEM((CHIPS + 1, NO, OWN, TO), BF16),
            pltpu.VMEM((3, PAIR, TO), F32),
            pltpu.VMEM((4, OWN, TO), BF16),
            pltpu.VMEM((NO, OWN, TO), BF16),
            pltpu.VMEM((GROUP, HEAD + 8, PAIR), F32),
            pltpu.VMEM((8, PAIR), F32),
            dma((NK,)),
            dma((2,)),
            dma,
            dma((CHIPS, NCH)),
            dma((CHIPS,)),
            dma((CHIPS,)),
            dma((2, CHIPS)),
            dma((CHIPS + 1, NO)),
            dma((CHIPS,)),
            dma((NO,)),
            dma((4,)),
            dma,
            dma,
            pltpu.SemaphoreType.REGULAR,
        ],
        compiler_params=pltpu.CompilerParams(collective_id=0, has_side_effects=True, vmem_limit_bytes=67043328),
        cost_estimate=pl.CostEstimate(flops=160 * 10**9, bytes_accessed=640 * 10**6, transcendentals=8 * 10**6),
    )(x, gain.reshape(1, D), cos, sin, wq, wk, wv, wo)
    return y


def solution(mesh):
    def step(x, gain, wq, wk, wv, wo):
        half = HEAD // 2
        angle = jnp.arange(ROWS, dtype=F32)[:, None] * THETA ** (-jnp.arange(half, dtype=F32) / half)
        cos, sin = jnp.cos(angle), jnp.sin(angle)
        y = layer(x, gain, jnp.concatenate([cos, cos], 1), jnp.concatenate([-sin, sin], 1), wq, wk, wv, wo)
        return (x.astype(F32) + y.astype(F32)).astype(BF16)

    tokens, columns = P(("dp", "tp"), None), P(None, "tp")
    return jax.shard_map(
        step,
        mesh=mesh,
        in_specs=(tokens, P(None), columns, columns, columns, P("tp", None)),
        out_specs=tokens,
        check_vma=False,
    )
```

```python
import functools

import jax
import jax.numpy as jnp
from jax import lax
from jax.experimental import pallas as pl
from jax.experimental.pallas import tpu as pltpu
from jax.sharding import PartitionSpec as P

HEAD = 128
THETA = 10000
D = 12288
ROWS = 1024
OWN = 128
PAIR = 256
CHIPS = 4
WIDE = 1536
HEADS = 12
TK = 1536
NK = D // TK
NORM = 16
TO = 1024
NO = D // TO
TP = 768
GROUP = 4
BLOCK = 256
LOG2E = 1.4426950408889634
HIDDEN = -2e30
MESH = pl.DeviceIdType.MESH
F32, BF16 = jnp.float32, jnp.bfloat16


def _dot(a, b, ca, cb):
    return lax.dot_general(a, b, (((ca,), (cb,)), ((), ())), preferred_element_type=F32)


def _loop(n, body):
    lax.fori_loop(0, n, lambda i, _: body(i), None)


def _kernel(x_ref, gain_ref, cos_ref, sin_ref, wq_ref, wk_ref, wv_ref, wo_ref, y_ref, all_ref, wring, xring, sums, nin, nout, kbuf, vbuf, qbuf, seen,
            oring, up, acc, stage, sib, mix_s, top_s, wsem, osem, insem, outsem, arrive, pair_recv, pair_send, line_send, sum_recv, sum_send, sib_recv,
            sib_send, ysem, xsem, free):
    tp = lax.axis_index("tp")
    z, c = lax.div(tp, 2), lax.rem(tp, 2)
    me_sib = {"tp": 2 * z + 1 - c}
    right = {"tp": jnp.minimum(tp + 2, 7)}
    left = {"tp": jnp.maximum(tp - 2, 0)}
    inner = (z > 0) & (z < 3)
    weights = (wq_ref, wk_ref, wv_ref)

    def fetch(p, kc):
        return pltpu.make_async_copy(weights[p].at[pl.ds(pl.multiple_of(kc * TK, TK), TK)], wring.at[p], wsem.at[p])

    def fetch_o(j, slot):
        return pltpu.make_async_copy(wo_ref.at[:, pl.ds(pl.multiple_of(j * TO, TO), TO)], oring.at[slot], osem.at[slot])

    def x_in(i):
        slot = lax.rem(i, 2)
        return pltpu.make_async_copy(x_ref.at[pl.ds(pl.multiple_of(i * NORM, NORM), NORM)], nin.at[slot], insem.at[slot])

    for i in range(2):
        x_in(i).start()
    for p in range(3):
        fetch(p, 0).start()
    for j in range(2):
        fetch_o(j, j).start()

    def part(s, core, kc):
        return all_ref.at[pl.ds(pl.multiple_of(s * PAIR + core * OWN, OWN), OWN), pl.ds(pl.multiple_of(kc * TK, TK), TK)]

    def to_sib(s, kc):
        return pltpu.make_async_remote_copy(src_ref=part(s, c, kc), dst_ref=part(s, c, kc), send_sem=pair_send.at[s], recv_sem=pair_recv.at[s, kc],
                                            device_id=me_sib, device_id_type=MESH)

    def along(s, kc, way):
        return pltpu.make_async_remote_copy(src_ref=part(s, c, kc), dst_ref=part(s, c, kc), send_sem=line_send.at[way, s], recv_sem=arrive.at[s, kc],
                                            device_id=left if way else right, device_id_type=MESH)

    def handle(s, kc):
        along(s, kc, 0).wait_recv()

        @pl.when((s < z) & (z < 3))
        def _():
            along(s, kc, 0).start()

        @pl.when((s > z) & (z > 0))
        def _():
            along(s, kc, 1).start()

        to_sib(s, kc).start()

    barrier = pltpu.get_barrier_semaphore()
    pl.semaphore_signal(barrier, inc=1, device_id=me_sib, device_id_type=MESH)

    @pl.when(z < 3)
    def _():
        pl.semaphore_signal(barrier, inc=1, device_id=right, device_id_type=MESH)

    @pl.when(z > 0)
    def _():
        pl.semaphore_signal(barrier, inc=1, device_id=left, device_id_type=MESH)

    def keep(i):
        slot = lax.rem(i, 2)
        mine = all_ref.at[pl.ds(pl.multiple_of(z * PAIR + c * OWN + i * NORM, NORM), NORM)]
        return pltpu.make_async_copy(nout.at[slot], mine, outsem.at[slot])

    def norm(i):
        slot = lax.rem(i, 2)
        x_in(i).wait()
        wide = nin[slot].astype(F32)
        scale = lax.rsqrt(jnp.mean(wide * wide, -1, keepdims=True) + 1e-6)

        @pl.when(i >= 2)
        def _():
            keep(i - 2).wait()

        nout[slot] = (wide * scale * gain_ref[...].astype(F32)).astype(BF16)

        @pl.when(i < OWN // NORM - 2)
        def _():
            x_in(i + 2).start()

        keep(i).start()

    _loop(OWN // NORM, norm)
    for i in range(2):
        keep(OWN // NORM - 2 + i).wait()

    @pl.when(inner)
    def _():
        pl.semaphore_wait(barrier, 3)

    @pl.when(jnp.logical_not(inner))
    def _():
        pl.semaphore_wait(barrier, 2)

    def send_own(kc):
        to_sib(z, kc).start()

        @pl.when(z > 0)
        def _():
            along(z, kc, 1).start()

        @pl.when(z == 0)
        def _():
            along(z, kc, 0).start()

    _loop(NK, send_own)

    def relay(t, kc):
        @pl.when((z == 1) & (t == 0) & ((kc == 3) | (kc == 5) | (kc == 7)))
        def _():
            handle(0, lax.div(kc - 3, 2))

        @pl.when((z == 2) & (t == 0) & ((kc == 5) | (kc == 7)))
        def _():
            handle(0, lax.div(kc - 5, 2))

        @pl.when((z == 1) & (t == 1))
        def _():
            handle(2, kc)

        @pl.when((z == 2) & (t == 1))
        def _():
            handle(3, kc)

        @pl.when((z == 1) & (t == 2) & (lax.rem(kc, 2) == 1))
        def _():
            handle(3, lax.div(kc - 1, 2))

    def project(t, s):
        early = jnp.where(z == 1, jnp.where(t == 1, 3, jnp.where(t == 2, NK, NK // 2)), jnp.where(z == 2, jnp.where(t == 1, 2, jnp.where(t == 2, 0, NK)), 0))

        def load(kc):
            slot = lax.rem(kc, 2)
            return pltpu.make_async_copy(all_ref.at[pl.ds(pl.multiple_of(s * PAIR, PAIR), PAIR), pl.ds(pl.multiple_of(kc * TK, TK), TK)],
                                         xring.at[slot], xsem.at[slot])

        def ready(kc):
            @pl.when((s != z) & (kc >= early))
            def _():
                handle(s, kc)

            relay(t, kc)
            theirs = part(s, 1 - c, kc)
            pltpu.make_async_remote_copy(src_ref=theirs, dst_ref=theirs, send_sem=pair_send.at[s], recv_sem=pair_recv.at[s, kc],
                                         device_id=me_sib, device_id_type=MESH).wait_recv()
            load(kc).start()

        sums[...] = jnp.zeros_like(sums)
        ready(0)

        def step(kc):
            @pl.when(kc < NK - 1)
            def _():
                ready(kc + 1)

            load(kc).wait()
            x = xring.at[lax.rem(kc, 2)]
            for p in range(3):
                fetch(p, kc).wait()
                for n in range(0, WIDE, TP):
                    sums[p, :, n : n + TP] += _dot(x[...], wring[p, :, n : n + TP], 1, 0)

                @pl.when((t < CHIPS - 1) | (kc < NK - 1))
                def _():
                    fetch(p, lax.rem(kc + 1, NK)).start()

        _loop(NK, step)

        @pl.when(inner & (t == z))
        def _():
            _loop(NK, lambda kc: along(z, kc, 0).start())

        here = pl.ds(pl.multiple_of(s * PAIR, PAIR), PAIR)
        own = (s == z).astype(jnp.int32)

        def head(h):
            at = pl.ds(pl.multiple_of(h * HEAD, HEAD), HEAD)
            cos, sin = cos_ref[here, :], sin_ref[here, :]

            def turned(p):
                one = sums[p, :, at].astype(BF16).astype(F32)
                return (one * cos + pltpu.roll(one, HEAD // 2, 1) * sin).astype(BF16)

            qbuf[own, :, at] = turned(0)
            kbuf[here, at] = turned(1)
            vbuf[at, here] = sums[2, :, at].astype(BF16).T

        _loop(HEADS, head)

    def attend(s):
        e = HEAD**-0.5 * LOG2E
        ones = jnp.ones((8, BLOCK), BF16)
        own = (s == z).astype(jnp.int32)

        def group(g):
            ats = [pl.ds(pl.multiple_of((g * GROUP + n) * HEAD, HEAD), HEAD) for n in range(GROUP)]

            def block(j, diagonal):
                keys = pl.ds(pl.multiple_of(j * BLOCK, BLOCK), BLOCK)
                scores = [_dot(kbuf[keys, at], qbuf[own, :, at], 1, 1) for at in ats]
                weights, keeps = [], []
                if diagonal:
                    ok = lax.broadcasted_iota(jnp.int32, (BLOCK, PAIR), 1) >= lax.broadcasted_iota(jnp.int32, (BLOCK, PAIR), 0)
                for n, sc in enumerate(scores):
                    if diagonal:
                        sc = jnp.where(ok, sc, HIDDEN)
                        top = sc.max(axis=0, keepdims=True)
                    else:
                        old = top_s[n : n + 1, :]
                        top = jnp.maximum(old, sc.max(axis=0, keepdims=True))
                        keeps.append(jnp.exp2((old - top) * e))
                    top_s[n : n + 1, :] = top
                    weights.append(jnp.exp2((sc - top) * e).astype(BF16))
                for n, (at, p) in enumerate(zip(ats, weights)):
                    values = jnp.concatenate([vbuf[at, keys], ones], axis=0)
                    new = _dot(values, p, 1, 0)
                    mix_s[n] = new if diagonal else mix_s[n] * keeps[n] + new

            block(s, True)
            lax.fori_loop(0, s, lambda j, _: block(j, False), None)
            for n, at in enumerate(ats):
                out = mix_s[n, :HEAD, :] * (1 / mix_s[n, HEAD : HEAD + 1, :])
                seen[pl.ds(pl.multiple_of(s * PAIR, PAIR), PAIR), at] = out.T.astype(BF16)

        _loop(HEADS // GROUP, group)

    def output(s, n):
        last = s == z
        ours = pl.ds(pl.multiple_of(c * OWN, OWN), OWN)
        theirs = pl.ds(pl.multiple_of((1 - c) * OWN, OWN), OWN)
        from_near = jnp.where(last, z < 3, inner)
        from_left = last & (z > 0)
        target = jnp.where((z + 1 == s), CHIPS, s)

        def swap(j):
            return pltpu.make_async_remote_copy(src_ref=stage.at[lax.rem(j, 4)], dst_ref=sib.at[j], send_sem=sib_send.at[lax.rem(j, 4)],
                                                recv_sem=sib_recv.at[j], device_id=me_sib, device_id_type=MESH)

        def onward(j, to):
            return pltpu.make_async_remote_copy(src_ref=up.at[s, j], dst_ref=up.at[target, j], send_sem=sum_send.at[s], recv_sem=sum_recv.at[target, j],
                                                device_id=to, device_id_type=MESH)

        def arrived(slot, j):
            pltpu.make_async_remote_copy(src_ref=up.at[slot, j], dst_ref=up.at[slot, j], send_sem=sum_send.at[s], recv_sem=sum_recv.at[slot, j],
                                         device_id=right, device_id_type=MESH).wait_recv()

        @pl.when(n > 0)
        def _():
            pl.semaphore_wait(free, 1)

        def step(j):
            @pl.when(j < NO)
            def _():
                slot = lax.rem(j, 2)
                fetch_o(0, slot).wait()

                @pl.when(j >= 4)
                def _():
                    swap(j).wait_send()

                a = lax.rem(j, 3)
                acc[a] = _dot(seen[pl.ds(pl.multiple_of(s * PAIR, PAIR), PAIR), :], oring[slot], 1, 0)
                stage[lax.rem(j, 4)] = acc[a, theirs, :].astype(BF16)

                @pl.when((n < 3) | (j < NO - 2))
                def _():
                    fetch_o(lax.rem(j + 2, NO), slot).start()

            @pl.when((j >= 2) & (j < NO + 2))
            def _():
                f = j - 2
                a = lax.rem(f, 3)
                pltpu.make_async_remote_copy(src_ref=stage.at[0], dst_ref=sib.at[f], send_sem=sib_send.at[0], recv_sem=sib_recv.at[f],
                                             device_id=me_sib, device_id_type=MESH).wait_recv()
                acc[a, ours, :] = acc[a, ours, :] + sib[f].astype(F32)

                @pl.when(from_near)
                def _():
                    arrived(s, f)
                    acc[a, ours, :] = acc[a, ours, :] + up[s, f].astype(F32)

                @pl.when(from_left)
                def _():
                    arrived(CHIPS, f)
                    acc[a, ours, :] = acc[a, ours, :] + up[CHIPS, f].astype(F32)

                up[s, f] = acc[a, ours, :].astype(BF16)

            @pl.when(j < NO)
            def _():
                swap(j).start()

            @pl.when(j >= 3)
            def _():
                f = j - 3

                @pl.when(z > s)
                def _():
                    onward(f, left).start()

                @pl.when(z < s)
                def _():
                    onward(f, right).start()

                @pl.when(last)
                def _():
                    pltpu.make_async_copy(up.at[s, f], y_ref.at[:, pl.ds(pl.multiple_of(f * TO, TO), TO)], ysem).start()

        _loop(NO + 3, step)
        for j in range(NO - 4, NO):
            swap(j).wait_send()

        @pl.when(n < 3)
        def _():
            pl.semaphore_signal(free, inc=1, device_id=me_sib, device_id_type=MESH)

    start = jnp.where(z == 1, 3, jnp.where(z == 2, 2, 1))

    def turn(st):
        @pl.when(st < CHIPS)
        def _():
            b = jnp.where(st == 0, z, jnp.where(st <= z, st - 1, st))
            project(st, b)

            @pl.when((b != z) | (z == 0))
            def _():
                attend(b)

        n = st - start

        @pl.when((n >= 0) & (n < 4))
        def _():
            order1 = jnp.where(n == 1, 2, jnp.where(n == 2, 1, n))
            order2 = jnp.where(n < 2, n, 5 - n)
            output(jnp.where(z == 0, lax.rem(n + 1, 4), jnp.where(z == 1, order1, jnp.where(z == 2, order2, n))), n)

        @pl.when((st == z) & (z > 0))
        def _():
            attend(z)

    _loop(7, turn)

    def drain(s):
        block = all_ref.at[pl.ds(0, OWN)]
        pltpu.make_async_remote_copy(src_ref=block, dst_ref=block, send_sem=pair_send.at[s], recv_sem=pair_recv.at[s, 0],
                                     device_id=me_sib, device_id_type=MESH).wait_send()

        @pl.when((s <= z) & (z < 3))
        def _():
            pltpu.make_async_remote_copy(src_ref=block, dst_ref=block, send_sem=line_send.at[0, s], recv_sem=pair_recv.at[s, 0],
                                         device_id=right, device_id_type=MESH).wait_send()

        @pl.when((s >= z) & (z > 0))
        def _():
            pltpu.make_async_remote_copy(src_ref=block, dst_ref=block, send_sem=line_send.at[1, s], recv_sem=pair_recv.at[s, 0],
                                         device_id=left, device_id_type=MESH).wait_send()

        @pl.when(s != z)
        def _():
            pltpu.make_async_remote_copy(src_ref=up.at[s], dst_ref=up.at[s], send_sem=sum_send.at[s], recv_sem=sum_recv.at[s, 0],
                                         device_id=right, device_id_type=MESH).wait_send()

    _loop(CHIPS, drain)
    pltpu.make_async_copy(all_ref.at[pl.ds(0, OWN)], y_ref, ysem).wait()


def layer(x, gain, cos, sin, wq, wk, wv, wo):
    anywhere, vmem = pl.BlockSpec(memory_space=pl.ANY), pl.BlockSpec(memory_space=pltpu.VMEM)
    dma = pltpu.SemaphoreType.DMA
    y, _ = pl.pallas_call(
        _kernel,
        in_specs=[anywhere, vmem, vmem, vmem, anywhere, anywhere, anywhere, anywhere],
        out_specs=[anywhere, anywhere],
        out_shape=[jax.ShapeDtypeStruct((OWN, D), BF16), jax.ShapeDtypeStruct((ROWS, D), BF16)],
        scratch_shapes=[
            pltpu.VMEM((3, TK, WIDE), BF16),
            pltpu.VMEM((2, PAIR, TK), BF16),
            pltpu.VMEM((3, PAIR, WIDE), F32),
            pltpu.VMEM((2, NORM, D), BF16),
            pltpu.VMEM((2, NORM, D), BF16),
            pltpu.VMEM((ROWS, WIDE), BF16),
            pltpu.VMEM((WIDE, ROWS), BF16),
            pltpu.VMEM((2, PAIR, WIDE), BF16),
            pltpu.VMEM((ROWS, WIDE), BF16),
            pltpu.VMEM((2, WIDE, TO), BF16),
            pltpu.VMEM((CHIPS + 1, NO, OWN, TO), BF16),
            pltpu.VMEM((3, PAIR, TO), F32),
            pltpu.VMEM((4, OWN, TO), BF16),
            pltpu.VMEM((NO, OWN, TO), BF16),
            pltpu.VMEM((GROUP, HEAD + 8, PAIR), F32),
            pltpu.VMEM((8, PAIR), F32),
            dma((3,)),
            dma((2,)),
            dma((2,)),
            dma((2,)),
            dma((CHIPS, NK)),
            dma((CHIPS, NK)),
            dma((CHIPS,)),
            dma((2, CHIPS)),
            dma((CHIPS + 1, NO)),
            dma((CHIPS,)),
            dma((NO,)),
            dma((4,)),
            dma,
            dma((2,)),
            pltpu.SemaphoreType.REGULAR,
        ],
        compiler_params=pltpu.CompilerParams(collective_id=0, has_side_effects=True, vmem_limit_bytes=67043328),
        cost_estimate=pl.CostEstimate(flops=160 * 10**9, bytes_accessed=640 * 10**6, transcendentals=8 * 10**6),
    )(x, gain.reshape(1, D), cos, sin, wq, wk, wv, wo)
    return y


def solution(mesh):
    def step(x, gain, wq, wk, wv, wo):
        half = HEAD // 2
        angle = jnp.arange(ROWS, dtype=F32)[:, None] * THETA ** (-jnp.arange(half, dtype=F32) / half)
        cos, sin = jnp.cos(angle), jnp.sin(angle)
        y = layer(x, gain, jnp.concatenate([cos, cos], 1), jnp.concatenate([-sin, sin], 1), wq, wk, wv, wo)
        return (x.astype(F32) + y.astype(F32)).astype(BF16)

    tokens, columns = P(("dp", "tp"), None), P(None, "tp")
    return jax.shard_map(
        step,
        mesh=mesh,
        in_specs=(tokens, P(None), columns, columns, columns, P("tp", None)),
        out_specs=tokens,
        check_vma=False,
    )
```

```python
import functools

import jax
import jax.numpy as jnp
from jax import lax
from jax.experimental import pallas as pl
from jax.experimental.pallas import tpu as pltpu
from jax.sharding import PartitionSpec as P

HEAD = 128
THETA = 10000
D = 12288
ROWS = 1024
OWN = 128
PAIR = 256
CHIPS = 4
WIDE = 1536
HEADS = 12
TK = 1536
NK = D // TK
NORM = 16
TO = 768
RING = 3
NO = D // TO
TP = 768
GROUP = 4
BLOCK = 256
LOG2E = 1.4426950408889634
HIDDEN = -2e30
MESH = pl.DeviceIdType.MESH
F32, BF16 = jnp.float32, jnp.bfloat16


def _dot(a, b, ca, cb):
    return lax.dot_general(a, b, (((ca,), (cb,)), ((), ())), preferred_element_type=F32)


def _loop(n, body):
    lax.fori_loop(0, n, lambda i, _: body(i), None)


def _kernel(x_ref, gain_ref, cos_ref, sin_ref, wq_ref, wk_ref, wv_ref, wo_ref, y_ref, all_ref, wring, xring, sums, nin, nout, kbuf, vbuf, qbuf, seen,
            oring, up, acc, stage, sib, mix_s, top_s, wsem, osem, insem, outsem, arrive, pair_recv, pair_send, line_send, sum_recv, sum_send, sib_recv,
            sib_send, ysem, xsem, free):
    tp = lax.axis_index("tp")
    z, c = lax.div(tp, 2), lax.rem(tp, 2)
    me_sib = {"tp": 2 * z + 1 - c}
    right = {"tp": jnp.minimum(tp + 2, 7)}
    left = {"tp": jnp.maximum(tp - 2, 0)}
    inner = (z > 0) & (z < 3)
    weights = (wq_ref, wk_ref, wv_ref)

    def fetch(p, kc):
        return pltpu.make_async_copy(weights[p].at[pl.ds(pl.multiple_of(kc * TK, TK), TK)], wring.at[p], wsem.at[p])

    def fetch_o(j, slot):
        return pltpu.make_async_copy(wo_ref.at[:, pl.ds(pl.multiple_of(j * TO, TO), TO)], oring.at[slot], osem.at[slot])

    def x_in(i):
        slot = lax.rem(i, 2)
        return pltpu.make_async_copy(x_ref.at[pl.ds(pl.multiple_of(i * NORM, NORM), NORM)], nin.at[slot], insem.at[slot])

    for i in range(2):
        x_in(i).start()
    for p in range(3):
        fetch(p, 0).start()
    for j in range(RING):
        fetch_o(j, j).start()

    def part(s, core, kc):
        return all_ref.at[pl.ds(pl.multiple_of(s * PAIR + core * OWN, OWN), OWN), pl.ds(pl.multiple_of(kc * TK, TK), TK)]

    def to_sib(s, kc):
        return pltpu.make_async_remote_copy(src_ref=part(s, c, kc), dst_ref=part(s, c, kc), send_sem=pair_send.at[s], recv_sem=pair_recv.at[s, kc],
                                            device_id=me_sib, device_id_type=MESH)

    def along(s, kc, way):
        return pltpu.make_async_remote_copy(src_ref=part(s, c, kc), dst_ref=part(s, c, kc), send_sem=line_send.at[way, s], recv_sem=arrive.at[s, kc],
                                            device_id=left if way else right, device_id_type=MESH)

    def handle(s, kc):
        along(s, kc, 0).wait_recv()

        @pl.when((s < z) & (z < 3))
        def _():
            along(s, kc, 0).start()

        @pl.when((s > z) & (z > 0))
        def _():
            along(s, kc, 1).start()

        to_sib(s, kc).start()

    barrier = pltpu.get_barrier_semaphore()
    pl.semaphore_signal(barrier, inc=1, device_id=me_sib, device_id_type=MESH)

    @pl.when(z < 3)
    def _():
        pl.semaphore_signal(barrier, inc=1, device_id=right, device_id_type=MESH)

    @pl.when(z > 0)
    def _():
        pl.semaphore_signal(barrier, inc=1, device_id=left, device_id_type=MESH)

    def keep(i):
        slot = lax.rem(i, 2)
        mine = all_ref.at[pl.ds(pl.multiple_of(z * PAIR + c * OWN + i * NORM, NORM), NORM)]
        return pltpu.make_async_copy(nout.at[slot], mine, outsem.at[slot])

    def norm(i):
        slot = lax.rem(i, 2)
        x_in(i).wait()
        wide = nin[slot].astype(F32)
        scale = lax.rsqrt(jnp.mean(wide * wide, -1, keepdims=True) + 1e-6)

        @pl.when(i >= 2)
        def _():
            keep(i - 2).wait()

        nout[slot] = (wide * scale * gain_ref[...].astype(F32)).astype(BF16)

        @pl.when(i < OWN // NORM - 2)
        def _():
            x_in(i + 2).start()

        keep(i).start()

    _loop(OWN // NORM, norm)
    for i in range(2):
        keep(OWN // NORM - 2 + i).wait()

    @pl.when(inner)
    def _():
        pl.semaphore_wait(barrier, 3)

    @pl.when(jnp.logical_not(inner))
    def _():
        pl.semaphore_wait(barrier, 2)

    def send_own(kc):
        to_sib(z, kc).start()

        @pl.when(z > 0)
        def _():
            along(z, kc, 1).start()

        @pl.when((z == 0) | (inner & (kc < z)))
        def _():
            along(z, kc, 0).start()

    _loop(NK, send_own)

    def relay(t, kc):
        @pl.when((z == 1) & (t == 0) & ((kc == 3) | (kc == 5) | (kc == 7)))
        def _():
            handle(0, lax.div(kc - 3, 2))

        @pl.when((z == 2) & (t == 0) & ((kc == 5) | (kc == 7)))
        def _():
            handle(0, lax.div(kc - 5, 2))

        @pl.when((z == 1) & (t == 1))
        def _():
            handle(2, kc)

        @pl.when((z == 2) & (t == 1))
        def _():
            handle(3, kc)

        @pl.when((z == 1) & (t == 2) & (lax.rem(kc, 2) == 1))
        def _():
            handle(3, lax.div(kc - 1, 2))

    def project(t, s):
        early = jnp.where(z == 1, jnp.where(t == 1, 3, jnp.where(t == 2, NK, NK // 2)), jnp.where(z == 2, jnp.where(t == 1, 2, jnp.where(t == 2, 0, NK)), 0))

        def load(kc):
            slot = lax.rem(kc, 2)
            return pltpu.make_async_copy(all_ref.at[pl.ds(pl.multiple_of(s * PAIR, PAIR), PAIR), pl.ds(pl.multiple_of(kc * TK, TK), TK)],
                                         xring.at[slot], xsem.at[slot])

        def ready(kc):
            @pl.when((s != z) & (kc >= early))
            def _():
                handle(s, kc)

            @pl.when(inner & (t == z) & (kc == NK - 1))
            def _():
                lax.fori_loop(z, NK, lambda k, _: along(z, k, 0).start(), None)

            relay(t, kc)
            theirs = part(s, 1 - c, kc)
            pltpu.make_async_remote_copy(src_ref=theirs, dst_ref=theirs, send_sem=pair_send.at[s], recv_sem=pair_recv.at[s, kc],
                                         device_id=me_sib, device_id_type=MESH).wait_recv()
            load(kc).start()

        sums[...] = jnp.zeros_like(sums)
        ready(0)

        def step(kc):
            @pl.when(kc < NK - 1)
            def _():
                ready(kc + 1)

            load(kc).wait()
            x = xring.at[lax.rem(kc, 2)]
            for p in range(3):
                fetch(p, kc).wait()
                for n in range(0, WIDE, TP):
                    sums[p, :, n : n + TP] += _dot(x[...], wring[p, :, n : n + TP], 1, 0)

                @pl.when((t < CHIPS - 1) | (kc < NK - 1))
                def _():
                    fetch(p, lax.rem(kc + 1, NK)).start()

        _loop(NK, step)

        here = pl.ds(pl.multiple_of(s * PAIR, PAIR), PAIR)
        own = (s == z).astype(jnp.int32)

        def head(h):
            at = pl.ds(pl.multiple_of(h * HEAD, HEAD), HEAD)
            cos, sin = cos_ref[here, :], sin_ref[here, :]

            def turned(p):
                one = sums[p, :, at].astype(BF16).astype(F32)
                return (one * cos + pltpu.roll(one, HEAD // 2, 1) * sin).astype(BF16)

            qbuf[own, :, at] = turned(0)
            kbuf[here, at] = turned(1)
            vbuf[at, here] = sums[2, :, at].astype(BF16).T

        _loop(HEADS, head)

    def attend(s):
        e = HEAD**-0.5 * LOG2E
        ones = jnp.ones((8, BLOCK), BF16)
        own = (s == z).astype(jnp.int32)

        def group(g):
            ats = [pl.ds(pl.multiple_of((g * GROUP + n) * HEAD, HEAD), HEAD) for n in range(GROUP)]

            def block(j, diagonal):
                keys = pl.ds(pl.multiple_of(j * BLOCK, BLOCK), BLOCK)
                scores = [_dot(kbuf[keys, at], qbuf[own, :, at], 1, 1) for at in ats]
                weights, keeps = [], []
                if diagonal:
                    ok = lax.broadcasted_iota(jnp.int32, (BLOCK, PAIR), 1) >= lax.broadcasted_iota(jnp.int32, (BLOCK, PAIR), 0)
                for n, sc in enumerate(scores):
                    if diagonal:
                        sc = jnp.where(ok, sc, HIDDEN)
                        top = sc.max(axis=0, keepdims=True)
                    else:
                        old = top_s[n : n + 1, :]
                        top = jnp.maximum(old, sc.max(axis=0, keepdims=True))
                        keeps.append(jnp.exp2((old - top) * e))
                    top_s[n : n + 1, :] = top
                    weights.append(jnp.exp2((sc - top) * e).astype(BF16))
                for n, (at, p) in enumerate(zip(ats, weights)):
                    values = jnp.concatenate([vbuf[at, keys], ones], axis=0)
                    new = _dot(values, p, 1, 0)
                    mix_s[n] = new if diagonal else mix_s[n] * keeps[n] + new

            block(s, True)
            lax.fori_loop(0, s, lambda j, _: block(j, False), None)
            for n, at in enumerate(ats):
                out = mix_s[n, :HEAD, :] * (1 / mix_s[n, HEAD : HEAD + 1, :])
                seen[pl.ds(pl.multiple_of(s * PAIR, PAIR), PAIR), at] = out.T.astype(BF16)

        _loop(HEADS // GROUP, group)

    def output(s, n):
        last = s == z
        ours = pl.ds(pl.multiple_of(c * OWN, OWN), OWN)
        theirs = pl.ds(pl.multiple_of((1 - c) * OWN, OWN), OWN)
        from_near = jnp.where(last, z < 3, inner)
        from_left = last & (z > 0)
        target = jnp.where((z + 1 == s), CHIPS, s)

        def swap(j):
            return pltpu.make_async_remote_copy(src_ref=stage.at[lax.rem(j, 4)], dst_ref=sib.at[j], send_sem=sib_send.at[lax.rem(j, 4)],
                                                recv_sem=sib_recv.at[j], device_id=me_sib, device_id_type=MESH)

        def onward(j, to):
            return pltpu.make_async_remote_copy(src_ref=up.at[s, j], dst_ref=up.at[target, j], send_sem=sum_send.at[s], recv_sem=sum_recv.at[target, j],
                                                device_id=to, device_id_type=MESH)

        def arrived(slot, j):
            pltpu.make_async_remote_copy(src_ref=up.at[slot, j], dst_ref=up.at[slot, j], send_sem=sum_send.at[s], recv_sem=sum_recv.at[slot, j],
                                         device_id=right, device_id_type=MESH).wait_recv()

        @pl.when(n > 0)
        def _():
            pl.semaphore_wait(free, 1)

        def step(j):
            @pl.when(j < NO)
            def _():
                slot = lax.rem(n * NO + j, RING)
                fetch_o(0, slot).wait()

                @pl.when(j >= 4)
                def _():
                    swap(j).wait_send()

                a = lax.rem(j, 3)
                acc[a] = _dot(seen[pl.ds(pl.multiple_of(s * PAIR, PAIR), PAIR), :], oring[slot], 1, 0)
                stage[lax.rem(j, 4)] = acc[a, theirs, :].astype(BF16)

                @pl.when((n < 3) | (j < NO - RING))
                def _():
                    fetch_o(lax.rem(j + RING, NO), slot).start()

            @pl.when((j >= 2) & (j < NO + 2))
            def _():
                f = j - 2
                a = lax.rem(f, 3)
                pltpu.make_async_remote_copy(src_ref=stage.at[0], dst_ref=sib.at[f], send_sem=sib_send.at[0], recv_sem=sib_recv.at[f],
                                             device_id=me_sib, device_id_type=MESH).wait_recv()

                def total():
                    return acc[a, ours, :] + sib[f].astype(F32)

                @pl.when(jnp.logical_not(from_near | from_left))
                def _():
                    up[s, f] = total().astype(BF16)

                @pl.when(from_near & jnp.logical_not(from_left))
                def _():
                    arrived(s, f)
                    up[s, f] = (total() + up[s, f].astype(F32)).astype(BF16)

                @pl.when(from_left & jnp.logical_not(from_near))
                def _():
                    arrived(CHIPS, f)
                    up[s, f] = (total() + up[CHIPS, f].astype(F32)).astype(BF16)

                @pl.when(from_left & from_near)
                def _():
                    arrived(s, f)
                    arrived(CHIPS, f)
                    up[s, f] = (total() + up[s, f].astype(F32) + up[CHIPS, f].astype(F32)).astype(BF16)

            @pl.when(j < NO)
            def _():
                swap(j).start()

            @pl.when((j >= 2) & (j < NO + 2))
            def _():
                f = j - 2

                @pl.when(z > s)
                def _():
                    onward(f, left).start()

                @pl.when(z < s)
                def _():
                    onward(f, right).start()

                @pl.when(last)
                def _():
                    pltpu.make_async_copy(up.at[s, f], y_ref.at[:, pl.ds(pl.multiple_of(f * TO, TO), TO)], ysem).start()

        _loop(NO + 2, step)
        for j in range(NO - 4, NO):
            swap(j).wait_send()

        @pl.when(n < 3)
        def _():
            pl.semaphore_signal(free, inc=1, device_id=me_sib, device_id_type=MESH)

    start = jnp.where(z == 1, 3, jnp.where(z == 2, 2, 1))

    def turn(st):
        @pl.when(st < CHIPS)
        def _():
            b = jnp.where(st == 0, z, jnp.where(st <= z, st - 1, st))
            project(st, b)

            @pl.when((b != z) | (z == 0))
            def _():
                attend(b)

        n = st - start

        @pl.when((n >= 0) & (n < 4))
        def _():
            order1 = jnp.where(n == 0, 2, jnp.where(n == 1, 0, jnp.where(n == 2, 3, 1)))
            order2 = jnp.where(n < 2, n, 5 - n)
            output(jnp.where(z == 0, lax.rem(n + 1, 4), jnp.where(z == 1, order1, jnp.where(z == 2, order2, n))), n)

        @pl.when((st == z) & (z > 0))
        def _():
            attend(z)

    _loop(7, turn)

    def drain(s):
        block = all_ref.at[pl.ds(0, OWN)]
        pltpu.make_async_remote_copy(src_ref=block, dst_ref=block, send_sem=pair_send.at[s], recv_sem=pair_recv.at[s, 0],
                                     device_id=me_sib, device_id_type=MESH).wait_send()

        @pl.when((s <= z) & (z < 3))
        def _():
            pltpu.make_async_remote_copy(src_ref=block, dst_ref=block, send_sem=line_send.at[0, s], recv_sem=pair_recv.at[s, 0],
                                         device_id=right, device_id_type=MESH).wait_send()

        @pl.when((s >= z) & (z > 0))
        def _():
            pltpu.make_async_remote_copy(src_ref=block, dst_ref=block, send_sem=line_send.at[1, s], recv_sem=pair_recv.at[s, 0],
                                         device_id=left, device_id_type=MESH).wait_send()

        @pl.when(s != z)
        def _():
            pltpu.make_async_remote_copy(src_ref=up.at[s], dst_ref=up.at[s], send_sem=sum_send.at[s], recv_sem=sum_recv.at[s, 0],
                                         device_id=right, device_id_type=MESH).wait_send()

    _loop(CHIPS, drain)
    pltpu.make_async_copy(all_ref.at[pl.ds(0, OWN)], y_ref, ysem).wait()


def layer(x, gain, cos, sin, wq, wk, wv, wo):
    anywhere, vmem = pl.BlockSpec(memory_space=pl.ANY), pl.BlockSpec(memory_space=pltpu.VMEM)
    dma = pltpu.SemaphoreType.DMA
    y, _ = pl.pallas_call(
        _kernel,
        in_specs=[anywhere, vmem, vmem, vmem, anywhere, anywhere, anywhere, anywhere],
        out_specs=[anywhere, anywhere],
        out_shape=[jax.ShapeDtypeStruct((OWN, D), BF16), jax.ShapeDtypeStruct((ROWS, D), BF16)],
        scratch_shapes=[
            pltpu.VMEM((3, TK, WIDE), BF16),
            pltpu.VMEM((2, PAIR, TK), BF16),
            pltpu.VMEM((3, PAIR, WIDE), F32),
            pltpu.VMEM((2, NORM, D), BF16),
            pltpu.VMEM((2, NORM, D), BF16),
            pltpu.VMEM((ROWS, WIDE), BF16),
            pltpu.VMEM((WIDE, ROWS), BF16),
            pltpu.VMEM((2, PAIR, WIDE), BF16),
            pltpu.VMEM((ROWS, WIDE), BF16),
            pltpu.VMEM((RING, WIDE, TO), BF16),
            pltpu.VMEM((CHIPS + 1, NO, OWN, TO), BF16),
            pltpu.VMEM((3, PAIR, TO), F32),
            pltpu.VMEM((4, OWN, TO), BF16),
            pltpu.VMEM((NO, OWN, TO), BF16),
            pltpu.VMEM((GROUP, HEAD + 8, PAIR), F32),
            pltpu.VMEM((8, PAIR), F32),
            dma((3,)),
            dma((RING,)),
            dma((2,)),
            dma((2,)),
            dma((CHIPS, NK)),
            dma((CHIPS, NK)),
            dma((CHIPS,)),
            dma((2, CHIPS)),
            dma((CHIPS + 1, NO)),
            dma((CHIPS,)),
            dma((NO,)),
            dma((4,)),
            dma,
            dma((2,)),
            pltpu.SemaphoreType.REGULAR,
        ],
        compiler_params=pltpu.CompilerParams(collective_id=0, has_side_effects=True, vmem_limit_bytes=67043328),
        cost_estimate=pl.CostEstimate(flops=160 * 10**9, bytes_accessed=640 * 10**6, transcendentals=8 * 10**6),
    )(x, gain.reshape(1, D), cos, sin, wq, wk, wv, wo)
    return y


def solution(mesh):
    def step(x, gain, wq, wk, wv, wo):
        half = HEAD // 2
        angle = jnp.arange(ROWS, dtype=F32)[:, None] * THETA ** (-jnp.arange(half, dtype=F32) / half)
        cos, sin = jnp.cos(angle), jnp.sin(angle)
        y = layer(x, gain, jnp.concatenate([cos, cos], 1), jnp.concatenate([-sin, sin], 1), wq, wk, wv, wo)
        return (x.astype(F32) + y.astype(F32)).astype(BF16)

    tokens, columns = P(("dp", "tp"), None), P(None, "tp")
    return jax.shard_map(
        step,
        mesh=mesh,
        in_specs=(tokens, P(None), columns, columns, columns, P("tp", None)),
        out_specs=tokens,
        check_vma=False,
    )
```
